32 devices in a mesh: groups: 2 (over x), ctx: 16 (over z, y, core).
Axes of the slice: x: 2, y: 2, z: 4, core: 2. Of those that a mesh axis runs over, the one named last changes fastest.
Arguments:
- queries: bfloat16 [256, 2048], P(('groups', 'ctx')), parts along dimension 0, may hold values from -200 to 200
- slab_keys: bfloat16 [256, 2048], P(('groups', 'ctx')), parts along dimension 0, may hold values from -6 to 6
- slab_values: bfloat16 [256, 2048], P(('groups', 'ctx')), parts along dimension 0, may hold values from -6 to 6
- cache_keys: bfloat16 [16384, 2048], P(('groups', 'ctx')), parts along dimension 0, may hold values from -12 to 12
- cache_values: bfloat16 [16384, 2048], P(('groups', 'ctx')), parts along dimension 0, may hold values from -6 to 6
- offset: int32 [2], P('groups'), parts along dimension 0, may hold values from 2048 to 8192
- slab_len: int32 [2], P('groups'), parts along dimension 0, may hold values from 64 to 128
Outputs:
- attended: bfloat16 [256, 2048], P(('groups', 'ctx')), parts along dimension 0
The draws below stay inside these ranges and needn't reach their ends.
There are 2 independent parts, one for each index of `groups`. The reference program is written for one: setup_inputs(seed, part) draws one part's arguments, and reference() takes and returns one part's arrays. A program takes and returns all parts, laid end to end along the dimension named above; each array names one. Nothing has to cross between parts.
All inputs are finite; a program needn't handle non-finite values.
Results may differ from the reference program's by a relative error of at most 0.0081.
Values may be sent and summed in bfloat16 or wider, within the bound.
A program may use at most 128 MiB of HBM per device.

```python
import jax
import jax.numpy as jnp
from jax import lax

H = 16
DH = 128
KB = 256
CACHE_DEV = 512
Q_DEV = 8
HD = 2048
CACHE = 8192
SLAB = 128
N_CTX = 16


def joint_draw(key):
    query_key = jax.random.fold_in(key, 11)
    cache_key = jax.random.fold_in(key, 12)
    query_draw = jnp.clip(jax.random.normal(query_key, (SLAB, HD), jnp.float32), -6.0, 6.0)
    key_draw = jnp.clip(jax.random.normal(cache_key, (CACHE, HD), jnp.float32), -6.0, 6.0)
    query_draw = 3.0 * query_draw
    return (query_draw, key_draw)


def draw_queries(key, part):
    return joint_draw(key)[0].astype(jnp.bfloat16)


def draw_cache_keys(key, part):
    return joint_draw(key)[1].astype(jnp.bfloat16)


def shard_levels(rng, shape, cuts, smallest, high):
    def one(position, shards_of):
        draws = jax.random.uniform(jax.random.fold_in(jax.random.fold_in(rng, 6), position), (shards_of,), jnp.float32, smallest / len(cuts), high / len(cuts))
        return jnp.repeat(jnp.exp(draws), shape[position] // shards_of).reshape((-1,) + (1,) * (len(shape) - position - 1))

    gain = one(*cuts[0])
    for cut in cuts[1:]:
        gain = gain * one(*cut)
    return gain


def noise(own_key, extent, spread, reach, pieces=(), held_as=jnp.bfloat16):
    drawn = spread * jax.random.normal(own_key, extent, jnp.float32)
    if pieces:
        drawn = drawn * shard_levels(own_key, extent, pieces, -0.22, 0.18)
    return jnp.clip(drawn, -reach, reach).astype(held_as)


def setup_inputs(seed: int = 0, part: int = 0) -> dict:
    arg_keys = jax.random.split(jax.random.key(seed), 8)
    part_keys = jax.random.split(jax.random.fold_in(arg_keys[7], part), 8)
    return {
        "queries": draw_queries(jax.random.fold_in(jax.random.fold_in(arg_keys[7], part), 71), part),
        "slab_keys": noise(part_keys[1], (SLAB, HD), 1.0, 6.0, ((0, 16),)),
        "slab_values": noise(part_keys[2], (SLAB, HD), 1.0, 6.0, ((0, 16),)),
        "cache_keys": draw_cache_keys(jax.random.fold_in(jax.random.fold_in(arg_keys[7], part), 71), part),
        "cache_values": noise(part_keys[4], (CACHE, HD), 1.0, 6.0, ((0, 16),)),
        "offset": jax.random.randint(part_keys[5], (1,), CACHE // 4, CACHE + 1).astype(jnp.int32),
        "slab_len": jax.random.randint(part_keys[6], (1,), SLAB // 2, SLAB + 1).astype(jnp.int32),
    }


very_low = -1e30


def block_terms(scores, visible, value_blocks):
    masked = jnp.where(visible, scores, very_low)
    maxima = jnp.max(masked, axis=2)
    weights = jnp.exp(jnp.where(visible, scores - maxima[:, :, None], -jnp.inf))
    totals = jnp.sum(weights, axis=2)
    rounded = lax.optimization_barrier(weights.astype(jnp.bfloat16))
    products = jnp.einsum('qgk,gkd->qgd', rounded.astype(jnp.float32), value_blocks.astype(jnp.float32))
    return maxima, totals, products


def by_heads(matrix, length):
    return matrix.reshape(length, H, DH).transpose(1, 0, 2)


def reference(queries, slab_keys, slab_values, cache_keys, cache_values, offset, slab_len):
    score_scale = DH ** -0.5
    per_segment = CACHE_DEV // KB
    row_index = jnp.arange(SLAB, dtype=jnp.int32)
    cache_index = jnp.arange(CACHE, dtype=jnp.int32)
    cache_visible = jnp.broadcast_to((cache_index < offset[0]).reshape(1, CACHE // KB, KB), (SLAB, CACHE // KB, KB))
    slab_visible = ((row_index[None, :] <= row_index[:, None]) & (row_index[None, :] < slab_len[0])).reshape(SLAB, N_CTX, Q_DEV)

    def per_head(operands):
        query_head, cache_key_head, cache_value_head, slab_key_head, slab_value_head = operands
        cache_scores = jnp.dot(query_head, cache_key_head.T, preferred_element_type=jnp.float32) * score_scale
        cache_max, cache_total, cache_sum = block_terms(cache_scores.reshape(SLAB, CACHE // KB, KB), cache_visible, cache_value_head.reshape(CACHE // KB, KB, DH))
        cache_max = cache_max.reshape(SLAB, N_CTX, per_segment)
        cache_total = cache_total.reshape(SLAB, N_CTX, per_segment)
        cache_sum = cache_sum.reshape(SLAB, N_CTX, per_segment, DH)
        segment_max = jnp.max(cache_max, axis=2)
        inner = jnp.exp(cache_max - segment_max[:, :, None])
        segment_total = jnp.sum(inner * cache_total, axis=2)
        segment_sum = jnp.sum(inner[..., None] * cache_sum, axis=2)
        quotient = segment_sum / jnp.maximum(segment_total, 1.0)[..., None]
        quotient = lax.optimization_barrier(quotient.astype(jnp.bfloat16)).astype(jnp.float32)
        slab_scores = jnp.dot(query_head, slab_key_head.T, preferred_element_type=jnp.float32) * score_scale
        slab_max, slab_total, slab_sum = block_terms(slab_scores.reshape(SLAB, N_CTX, Q_DEV), slab_visible, slab_value_head.reshape(N_CTX, Q_DEV, DH))
        maxima = jnp.concatenate([segment_max, slab_max], axis=1)
        totals = jnp.concatenate([segment_total, slab_total], axis=1)
        products = jnp.concatenate([segment_total[..., None] * quotient, slab_sum], axis=1)
        largest = jnp.max(maxima, axis=1)
        factors = jnp.exp(maxima - largest[:, None])
        numerator = jnp.sum(factors[:, :, None] * products, axis=1)
        denominator = jnp.sum(factors * totals, axis=1)
        return numerator / denominator[:, None]

    heads_out = lax.map(per_head, (by_heads(queries, SLAB), by_heads(cache_keys, CACHE), by_heads(cache_values, CACHE), by_heads(slab_keys, SLAB), by_heads(slab_values, SLAB)))
    merged = heads_out.transpose(1, 0, 2).reshape(SLAB, H * DH)
    merged = jnp.where((row_index < slab_len[0])[:, None], merged, 0.0)
    return merged.astype(jnp.bfloat16)
```

```python
import functools
import math

import jax
import jax.numpy as jnp
from jax import lax
from jax.experimental import pallas as pl
from jax.experimental.pallas import tpu as pltpu
from jax.sharding import PartitionSpec as P

DH = 128
LOWEST = -1e30
FLOOR = -1e29
EXP_SCALE = DH ** (-0.5) * math.log2(math.e)
GROUP_HEADS = 2


def kernel(
    n, offset_ref, slab_len_ref, q_ref, sk_ref, sv_ref, ck_ref, cv_ref, out_ref,
    qb, kb, vb, skb, svb, qs, sks, svs, ob, rb, sb, rs, fs, fr,
    local_sem, pair_send, pair_recv, q_send, q_recv, o_send, o_recv, s_send, s_recv,
):
    me = lax.axis_index("ctx")
    core = lax.rem(me, 2)
    other = 1 - core
    chip = lax.div(me, 2)
    chips = n // 2
    own_rows, width = q_ref.shape
    half = width // 2
    cache_rows = ck_ref.shape[0]
    chip_rows = 2 * own_rows
    slab_rows = n * own_rows
    heads = half // DH
    groups = heads // GROUP_HEADS
    mine = pl.ds(pl.multiple_of(core * half, half), half)
    theirs = pl.ds(pl.multiple_of(other * half, half), half)
    key_rows = pl.ds(pl.multiple_of(core * cache_rows, cache_rows), cache_rows)
    partner = {"ctx": chip * 2 + other}

    def peer(step):
        return {"ctx": lax.rem(chip + step, chips) * 2 + core}

    moves = (
        (q_ref, qb.at[chip, core]),
        (ck_ref, kb.at[key_rows]),
        (cv_ref, vb.at[key_rows]),
        (sk_ref, skb.at[core]),
        (sv_ref, svb.at[core]),
    )
    local = [
        pltpu.make_async_copy(src.at[:, mine], dst, local_sem.at[i])
        for i, (src, dst) in enumerate(moves)
    ]
    for copy in local:
        copy.start()

    barrier = pltpu.get_barrier_semaphore()
    pl.semaphore_signal(barrier, inc=1, device_id=partner, device_id_type=pl.DeviceIdType.MESH)
    for step in range(1, chips):
        pl.semaphore_signal(
            barrier, inc=1, device_id=peer(step), device_id_type=pl.DeviceIdType.MESH
        )
    pl.semaphore_wait(barrier, chips)

    pair = [
        pltpu.make_async_remote_copy(
            src_ref=src.at[:, theirs], dst_ref=dst,
            send_sem=pair_send.at[i], recv_sem=pair_recv.at[i],
            device_id=partner, device_id_type=pl.DeviceIdType.MESH,
        )
        for i, (src, dst) in enumerate(moves)
    ]
    for copy in pair:
        copy.start()

    def send(src, dst, send_sem, recv_sem, device):
        copy = pltpu.make_async_remote_copy(
            src_ref=src, dst_ref=dst, send_sem=send_sem, recv_sem=recv_sem,
            device_id=device, device_id_type=pl.DeviceIdType.MESH,
        )
        copy.start()
        return copy

    local[0].wait()
    pair[0].wait()
    q_copies = [
        send(qb.at[chip], qb.at[chip], q_send.at[step], q_recv.at[step], peer(step))
        for step in range(1, chips)
    ]
    for copy in local[1:] + pair[1:]:
        copy.wait()
    sks[...] = skb[...].astype(jnp.float32).reshape(chip_rows, half).astype(jnp.bfloat16)
    svs[...] = svb[...].astype(jnp.float32).reshape(chip_rows, half).astype(jnp.bfloat16)
    offset = offset_ref[0]
    slab_len = slab_len_ref[0]
    position = chip * (2 * cache_rows) + lax.broadcasted_iota(jnp.int32, (1, 2 * cache_rows), 1)
    cache_bias = jnp.where(position < offset, 0.0, LOWEST)
    row = lax.broadcasted_iota(jnp.int32, (slab_rows, chip_rows), 0)
    column = chip * chip_rows + lax.broadcasted_iota(jnp.int32, (slab_rows, chip_rows), 1)
    slab_bias = jnp.where((column <= row) & (column < slab_len), 0.0, LOWEST)
    lane = lax.broadcasted_iota(jnp.int32, (slab_rows, DH), 1)

    for copy in q_copies:
        copy.wait()
    qs[...] = qb[...].astype(jnp.float32).reshape(slab_rows, half).astype(jnp.bfloat16)

    across = (((1,), (1,)), ((), ()))
    stats = jnp.zeros((slab_rows, DH), jnp.float32)
    o_copies = []
    for group in range(groups):
        for inner in range(GROUP_HEADS):
            h = group * GROUP_HEADS + inner
            cols = slice(h * DH, (h + 1) * DH)
            q = qs[:, cols]
            scores = lax.dot_general(
                q, kb[:, cols], across, preferred_element_type=jnp.float32
            ) + cache_bias
            slab_scores = lax.dot_general(
                q, sks[:, cols], across, preferred_element_type=jnp.float32
            ) + slab_bias
            largest = jnp.maximum(
                jnp.max(scores, axis=1, keepdims=True),
                jnp.max(slab_scores, axis=1, keepdims=True),
            )
            largest = jnp.maximum(largest, FLOOR)
            weights = jnp.exp2((scores - largest) * EXP_SCALE)
            slab_weights = jnp.exp2((slab_scores - largest) * EXP_SCALE)
            total = jnp.sum(weights, axis=1, keepdims=True) + jnp.sum(
                slab_weights, axis=1, keepdims=True
            )
            summed = jnp.dot(
                weights.astype(jnp.bfloat16), vb[:, cols], preferred_element_type=jnp.float32
            ) + jnp.dot(
                slab_weights.astype(jnp.bfloat16), svs[:, cols],
                preferred_element_type=jnp.float32,
            )
            stats = jnp.where(lane == h, largest, stats)
            stats = jnp.where(lane == heads + h, total, stats)
            ob[group, :, :, inner * DH : (inner + 1) * DH] = summed.reshape(
                chips, chip_rows, DH
            ).astype(jnp.bfloat16)
        for step in range(1, chips):
            target = lax.rem(chip + step, chips)
            o_copies.append(
                send(
                    ob.at[group, target], rb.at[group, step],
                    o_send.at[group, step], o_recv.at[group, step], peer(step),
                )
            )
    sb[...] = stats.reshape(chips, chip_rows, DH)
    s_copies = []
    for step in range(1, chips):
        target = lax.rem(chip + step, chips)
        s_copies.append(
            send(sb.at[target], rs.at[step], s_send.at[step], s_recv.at[step], peer(step))
        )
    for copy in s_copies:
        copy.wait()
    parts = [sb[chip]] + [rs[step] for step in range(1, chips)]
    top = functools.reduce(jnp.maximum, parts)
    factors = [jnp.exp2(jnp.minimum(part - top, 0.0) * EXP_SCALE) for part in parts]
    denominator = sum(
        factor * pltpu.roll(part, DH - heads, 1) for factor, part in zip(factors, parts)
    )
    inverse = 1.0 / denominator
    shares = [factor * inverse for factor in factors]
    out_row = chip * chip_rows + lax.broadcasted_iota(jnp.int32, (chip_rows, DH), 0)
    valid = out_row < slab_len
    for copy in o_copies:
        copy.wait()
    for h in range(heads):
        group, inner = divmod(h, GROUP_HEADS)
        cols = slice(inner * DH, (inner + 1) * DH)
        mixed = shares[0][:, h : h + 1] * ob[group, chip, :, cols].astype(jnp.float32)
        for step in range(1, chips):
            mixed = mixed + shares[step][:, h : h + 1] * rb[group, step, :, cols].astype(
                jnp.float32
            )
        mixed = jnp.where(valid, mixed, 0.0)
        fs[:, :, h * DH : (h + 1) * DH] = mixed.reshape(2, own_rows, DH).astype(jnp.bfloat16)
    last = send(
        fs.at[other], fr, pair_send.at[len(moves)], pair_recv.at[len(moves)], partner
    )
    out_ref[:, mine] = fs[core]
    last.wait()
    out_ref[:, theirs] = fr[...]


def body(queries, slab_keys, slab_values, cache_keys, cache_values, offset, slab_len):
    n = lax.axis_size("ctx")
    own_rows, width = queries.shape
    cache_rows = cache_keys.shape[0]
    chips, half, chip_rows = n // 2, width // 2, 2 * own_rows
    groups = half // DH // GROUP_HEADS
    wide = GROUP_HEADS * DH
    bf16, f32 = jnp.bfloat16, jnp.float32
    dma = pltpu.SemaphoreType.DMA
    vmem = pl.BlockSpec(memory_space=pltpu.VMEM)
    smem = pl.BlockSpec(memory_space=pltpu.SMEM)
    hbm = pl.BlockSpec(memory_space=pl.ANY)
    return pl.pallas_call(
        functools.partial(kernel, n),
        out_shape=jax.ShapeDtypeStruct(queries.shape, queries.dtype),
        in_specs=[smem, smem, vmem, vmem, vmem, hbm, hbm],
        out_specs=vmem,
        scratch_shapes=[
            pltpu.VMEM((chips, 2, own_rows, half), bf16),
            pltpu.VMEM((2 * cache_rows, half), bf16),
            pltpu.VMEM((2 * cache_rows, half), bf16),
            pltpu.VMEM((2, own_rows, half), bf16),
            pltpu.VMEM((2, own_rows, half), bf16),
            pltpu.VMEM((n * own_rows, half), bf16),
            pltpu.VMEM((chip_rows, half), bf16),
            pltpu.VMEM((chip_rows, half), bf16),
            pltpu.VMEM((groups, chips, chip_rows, wide), bf16),
            pltpu.VMEM((groups, chips, chip_rows, wide), bf16),
            pltpu.VMEM((chips, chip_rows, DH), f32),
            pltpu.VMEM((chips, chip_rows, DH), f32),
            pltpu.VMEM((2, own_rows, half), bf16),
            pltpu.VMEM((own_rows, half), bf16),
            dma((5,)),
            dma((6,)),
            dma((6,)),
            dma((chips,)),
            dma((chips,)),
            dma((groups, chips)),
            dma((groups, chips)),
            dma((chips,)),
            dma((chips,)),
        ],
        compiler_params=pltpu.CompilerParams(collective_id=0, has_side_effects=True),
    )(offset, slab_len, queries, slab_keys, slab_values, cache_keys, cache_values)


def solution(mesh):
    rows = P(("groups", "ctx"), None)
    placed = (rows, rows, rows, rows, rows, P("groups"), P("groups"))
    return jax.shard_map(
        body, mesh=mesh, in_specs=placed, out_specs=rows, check_vma=False
    )
```

```python
import functools
import math

import jax
import jax.numpy as jnp
from jax import lax
from jax.experimental import pallas as pl
from jax.experimental.pallas import tpu as pltpu
from jax.sharding import PartitionSpec as P

DH = 128
LOWEST = -1e30
FLOOR = -1e29
EXP_SCALE = DH ** (-0.5) * math.log2(math.e)
GROUP_HEADS = 2


def kernel(
    n, offset_ref, slab_len_ref, q_ref, sk_ref, sv_ref, ck_ref, cv_ref, out_ref,
    qb, kb, vb, skb, svb, qs, sks, svs, ob, rb, sb, rs, fs, fr,
    local_sem, pair_send, pair_recv, q_send, q_recv, o_send, o_recv, s_send, s_recv,
):
    me = lax.axis_index("ctx")
    core = lax.rem(me, 2)
    other = 1 - core
    chip = lax.div(me, 2)
    chips = n // 2
    own_rows, width = q_ref.shape
    half = width // 2
    cache_rows = ck_ref.shape[0]
    chip_rows = 2 * own_rows
    slab_rows = n * own_rows
    heads = half // DH
    groups = heads // GROUP_HEADS
    mine = pl.ds(pl.multiple_of(core * half, half), half)
    theirs = pl.ds(pl.multiple_of(other * half, half), half)
    key_rows = pl.ds(pl.multiple_of(core * cache_rows, cache_rows), cache_rows)
    partner = {"ctx": chip * 2 + other}

    def peer(step):
        return {"ctx": lax.rem(chip + step, chips) * 2 + core}

    wide = GROUP_HEADS * DH

    def part(base, group):
        return pl.ds(pl.multiple_of(base * half + group * wide, wide), wide)

    q_moves = [(q_ref, qb.at[group, chip, core], group) for group in range(groups)]
    moves = (
        (ck_ref, kb.at[key_rows]),
        (cv_ref, vb.at[key_rows]),
        (sk_ref, skb.at[core]),
        (sv_ref, svb.at[core]),
    )
    q_local = [
        pltpu.make_async_copy(src.at[:, part(core, group)], dst, local_sem.at[len(moves) + group])
        for src, dst, group in q_moves
    ]
    for copy in q_local:
        copy.start()
    local = [
        pltpu.make_async_copy(src.at[:, mine], dst, local_sem.at[i])
        for i, (src, dst) in enumerate(moves)
    ]
    for copy in local:
        copy.start()

    barrier = pltpu.get_barrier_semaphore()
    pl.semaphore_signal(barrier, inc=1, device_id=partner, device_id_type=pl.DeviceIdType.MESH)
    for step in range(1, chips):
        pl.semaphore_signal(
            barrier, inc=1, device_id=peer(step), device_id_type=pl.DeviceIdType.MESH
        )
    pl.semaphore_wait(barrier, chips)

    def send(src, dst, send_sem, recv_sem, device):
        copy = pltpu.make_async_remote_copy(
            src_ref=src, dst_ref=dst, send_sem=send_sem, recv_sem=recv_sem,
            device_id=device, device_id_type=pl.DeviceIdType.MESH,
        )
        copy.start()
        return copy

    q_pair = [
        send(
            src.at[:, part(other, group)], dst,
            pair_send.at[len(moves) + group], pair_recv.at[len(moves) + group], partner,
        )
        for src, dst, group in q_moves
    ]
    pair = [
        pltpu.make_async_remote_copy(
            src_ref=src.at[:, theirs], dst_ref=dst,
            send_sem=pair_send.at[i], recv_sem=pair_recv.at[i],
            device_id=partner, device_id_type=pl.DeviceIdType.MESH,
        )
        for i, (src, dst) in enumerate(moves)
    ]
    for copy in pair:
        copy.start()

    q_copies = []
    for group in range(groups):
        q_local[group].wait()
        q_pair[group].wait()
        q_copies.append(
            [
                send(
                    qb.at[group, chip], qb.at[group, chip],
                    q_send.at[group, step], q_recv.at[group, step], peer(step),
                )
                for step in range(1, chips)
            ]
        )
    for copy in local + pair:
        copy.wait()
    sks[...] = skb[...].astype(jnp.float32).reshape(chip_rows, half).astype(jnp.bfloat16)
    svs[...] = svb[...].astype(jnp.float32).reshape(chip_rows, half).astype(jnp.bfloat16)
    offset = offset_ref[0]
    slab_len = slab_len_ref[0]
    position = chip * (2 * cache_rows) + lax.broadcasted_iota(jnp.int32, (1, 2 * cache_rows), 1)
    cache_bias = jnp.where(position < offset, 0.0, LOWEST)
    row = lax.broadcasted_iota(jnp.int32, (slab_rows, chip_rows), 0)
    column = chip * chip_rows + lax.broadcasted_iota(jnp.int32, (slab_rows, chip_rows), 1)
    slab_bias = jnp.where((column <= row) & (column < slab_len), 0.0, LOWEST)
    lane = lax.broadcasted_iota(jnp.int32, (slab_rows, DH), 1)

    across = (((1,), (1,)), ((), ()))
    stats = jnp.zeros((slab_rows, DH), jnp.float32)
    o_copies = []
    for group in range(groups):
        for copy in q_copies[group]:
            copy.wait()
        qs[...] = qb[group].astype(jnp.float32).reshape(slab_rows, wide).astype(jnp.bfloat16)
        for inner in range(GROUP_HEADS):
            h = group * GROUP_HEADS + inner
            cols = slice(h * DH, (h + 1) * DH)
            q = qs[:, inner * DH : (inner + 1) * DH]
            scores = lax.dot_general(
                q, kb[:, cols], across, preferred_element_type=jnp.float32
            ) + cache_bias
            slab_scores = lax.dot_general(
                q, sks[:, cols], across, preferred_element_type=jnp.float32
            ) + slab_bias
            largest = jnp.maximum(
                jnp.max(scores, axis=1, keepdims=True),
                jnp.max(slab_scores, axis=1, keepdims=True),
            )
            largest = jnp.maximum(largest, FLOOR)
            weights = jnp.exp2((scores - largest) * EXP_SCALE)
            slab_weights = jnp.exp2((slab_scores - largest) * EXP_SCALE)
            total = jnp.sum(weights, axis=1, keepdims=True) + jnp.sum(
                slab_weights, axis=1, keepdims=True
            )
            summed = jnp.dot(
                weights.astype(jnp.bfloat16), vb[:, cols], preferred_element_type=jnp.float32
            ) + jnp.dot(
                slab_weights.astype(jnp.bfloat16), svs[:, cols],
                preferred_element_type=jnp.float32,
            )
            stats = jnp.where(lane == h, largest, stats)
            stats = jnp.where(lane == heads + h, total, stats)
            ob[group, :, :, inner * DH : (inner + 1) * DH] = summed.reshape(
                chips, chip_rows, DH
            ).astype(jnp.bfloat16)
        for step in range(1, chips):
            target = lax.rem(chip + step, chips)
            o_copies.append(
                send(
                    ob.at[group, target], rb.at[group, step],
                    o_send.at[group, step], o_recv.at[group, step], peer(step),
                )
            )
    stats = stats.reshape(chips, 2, own_rows, DH)
    low = lax.broadcasted_iota(jnp.int32, (chips, own_rows, DH), 2) < DH // 2
    sb[...] = jnp.where(low, stats[:, 0], pltpu.roll(stats[:, 1], DH // 2, 2))
    s_copies = []
    for step in range(1, chips):
        target = lax.rem(chip + step, chips)
        s_copies.append(
            send(sb.at[target], rs.at[step], s_send.at[step], s_recv.at[step], peer(step))
        )
    for copy in s_copies:
        copy.wait()
    parts = [sb[chip]] + [rs[step] for step in range(1, chips)]
    top = functools.reduce(jnp.maximum, parts)
    factors = [jnp.exp2(jnp.minimum(part - top, 0.0) * EXP_SCALE) for part in parts]
    denominator = sum(
        factor * pltpu.roll(part, DH - heads, 1) for factor, part in zip(factors, parts)
    )
    inverse = 1.0 / denominator
    shares = [factor * inverse for factor in factors]
    shares = [
        jnp.concatenate([share, pltpu.roll(share, DH // 2, 1)], axis=0) for share in shares
    ]
    out_row = chip * chip_rows + lax.broadcasted_iota(jnp.int32, (chip_rows, DH), 0)
    valid = out_row < slab_len
    for copy in o_copies:
        copy.wait()
    for h in range(heads):
        group, inner = divmod(h, GROUP_HEADS)
        cols = slice(inner * DH, (inner + 1) * DH)
        mixed = shares[0][:, h : h + 1] * ob[group, chip, :, cols].astype(jnp.float32)
        for step in range(1, chips):
            mixed = mixed + shares[step][:, h : h + 1] * rb[group, step, :, cols].astype(
                jnp.float32
            )
        mixed = jnp.where(valid, mixed, 0.0)
        fs[:, :, h * DH : (h + 1) * DH] = mixed.reshape(2, own_rows, DH).astype(jnp.bfloat16)
    last = send(
        fs.at[other], fr, pair_send.at[len(moves) + groups], pair_recv.at[len(moves) + groups], partner
    )
    out_ref[:, mine] = fs[core]
    last.wait()
    out_ref[:, theirs] = fr[...]


def body(queries, slab_keys, slab_values, cache_keys, cache_values, offset, slab_len):
    n = lax.axis_size("ctx")
    own_rows, width = queries.shape
    cache_rows = cache_keys.shape[0]
    chips, half, chip_rows = n // 2, width // 2, 2 * own_rows
    groups = half // DH // GROUP_HEADS
    wide = GROUP_HEADS * DH
    bf16, f32 = jnp.bfloat16, jnp.float32
    dma = pltpu.SemaphoreType.DMA
    vmem = pl.BlockSpec(memory_space=pltpu.VMEM)
    smem = pl.BlockSpec(memory_space=pltpu.SMEM)
    hbm = pl.BlockSpec(memory_space=pl.ANY)
    return pl.pallas_call(
        functools.partial(kernel, n),
        out_shape=jax.ShapeDtypeStruct(queries.shape, queries.dtype),
        in_specs=[smem, smem, vmem, vmem, vmem, hbm, hbm],
        out_specs=vmem,
        scratch_shapes=[
            pltpu.VMEM((groups, chips, 2, own_rows, wide), bf16),
            pltpu.VMEM((2 * cache_rows, half), bf16),
            pltpu.VMEM((2 * cache_rows, half), bf16),
            pltpu.VMEM((2, own_rows, half), bf16),
            pltpu.VMEM((2, own_rows, half), bf16),
            pltpu.VMEM((n * own_rows, wide), bf16),
            pltpu.VMEM((chip_rows, half), bf16),
            pltpu.VMEM((chip_rows, half), bf16),
            pltpu.VMEM((groups, chips, chip_rows, wide), bf16),
            pltpu.VMEM((groups, chips, chip_rows, wide), bf16),
            pltpu.VMEM((chips, own_rows, DH), f32),
            pltpu.VMEM((chips, own_rows, DH), f32),
            pltpu.VMEM((2, own_rows, half), bf16),
            pltpu.VMEM((own_rows, half), bf16),
            dma((4 + groups,)),
            dma((5 + groups,)),
            dma((5 + groups,)),
            dma((groups, chips)),
            dma((groups, chips)),
            dma((groups, chips)),
            dma((groups, chips)),
            dma((chips,)),
            dma((chips,)),
        ],
        compiler_params=pltpu.CompilerParams(collective_id=0, has_side_effects=True),
    )(offset, slab_len, queries, slab_keys, slab_values, cache_keys, cache_values)


def solution(mesh):
    rows = P(("groups", "ctx"), None)
    placed = (rows, rows, rows, rows, rows, P("groups"), P("groups"))
    return jax.shard_map(
        body, mesh=mesh, in_specs=placed, out_specs=rows, check_vma=False
    )
```
